32 devices in a mesh: gx: 2 (over y), gy: 4 (over z), gz: 4 (over x, core).
Axes of the slice: x: 2, y: 2, z: 4, core: 2. Of those that a mesh axis runs over, the one named last changes fastest.
Arguments:
- kappa_sq: float32 [32, 64, 512], P('gx', 'gz', 'gy'), may hold values from 0.004 to 0.4
- probe_bits: int32 [4, 32, 64, 512], P(None, 'gx', 'gz', 'gy'), may hold values from 0 to 1
Outputs:
- solution: float32 [4, 32, 64, 512], P(None, 'gx', 'gz', 'gy')
- relative_residual: float32 [4], replicated
The draws below stay inside these ranges and needn't reach their ends.
All inputs are finite; a program needn't handle non-finite values.
Results may differ from the reference program's by a relative error of at most 0.0001.
Values sent between devices are 32-bit elements; how exact they have to be, the bound alone decides.
A program may use at most 128 MiB of HBM per device.

```python
import math
import jax
import jax.numpy as jnp
from jax import lax

PROBES = 4
LEVELS = 3
COARSE_SWEEPS = 8
ITERS = 2
NX = 32
NZ = 64
NY = 512


def place_ends(array, own_key, smallest, top_value):
    place = [jax.random.randint(jax.random.fold_in(own_key, axis), (), 0, length) for axis, length in enumerate(array.shape)]
    main_axis = array.shape.index(max(array.shape))
    beside = place[:main_axis] + [(place[main_axis] + 1) % array.shape[main_axis]] + place[main_axis + 1:]
    return array.at[tuple(place)].set(smallest).at[tuple(beside)].set(top_value)


def shard_levels(stream_key, dims, cuts, low, high):
    def one(dim, shards_of):
        draws = jax.random.uniform(jax.random.fold_in(jax.random.fold_in(stream_key, 6), dim), (shards_of,), jnp.float32, low / len(cuts), high / len(cuts))
        return jnp.repeat(jnp.exp(draws), dims[dim] // shards_of).reshape((-1,) + (1,) * (len(dims) - dim - 1))

    level = one(*cuts[0])
    for cut in cuts[1:]:
        level = level * one(*cut)
    return level


def setup_inputs(seed: int = 0) -> dict:
    arg_keys = jax.random.split(jax.random.key(seed), 3)
    kappa_sq = jnp.clip(jnp.exp(math.log(0.4) - 4.6051702 * jax.random.uniform(arg_keys[0], (NX, NZ, NY), jnp.float32) ** shard_levels(arg_keys[0], (NX, NZ, NY), ((0, 2), (1, 4), (2, 4)), -0.2, 0.2)), 0.004, 0.4)
    probe_bits = place_ends(jax.random.randint(arg_keys[1], (PROBES, NX, NZ, NY), 0, 2), jax.random.fold_in(arg_keys[1], 1), 0, 1).astype(jnp.int32)
    return {"kappa_sq": kappa_sq, "probe_bits": probe_bits}


damping = 0.8

def neighbours(padded):
    along_first = padded[..., 2:, 1:-1, 1:-1] + padded[..., :-2, 1:-1, 1:-1]
    along_second = padded[..., 1:-1, 2:, 1:-1] + padded[..., 1:-1, :-2, 1:-1]
    along_third = padded[..., 1:-1, 1:-1, 2:] + padded[..., 1:-1, 1:-1, :-2]
    return along_first + along_second + along_third

def coarsen(field):
    leading = field.shape[:-3]
    cells_first, cells_second, cells_third = field.shape[-3:]
    grouped = field.reshape(leading + (cells_first // 2, 2, cells_second // 2, 2, cells_third // 2, 2))
    return lax.optimization_barrier(jnp.mean(grouped, axis=(-5, -3, -1)))

def refine(field):
    leading = field.shape[:-3]
    cells_first, cells_second, cells_third = field.shape[-3:]
    spread = field.reshape(leading + (cells_first, 1, cells_second, 1, cells_third, 1))
    spread = jnp.broadcast_to(spread, leading + (cells_first, 2, cells_second, 2, cells_third, 2))
    return spread.reshape(leading + (cells_first * 2, cells_second * 2, cells_third * 2))

def reference(kappa_sq, probe_bits):
    diagonals = []
    couplings = []
    coef_field = kappa_sq
    for grid_level in range(LEVELS + 1):
        if grid_level > 0:
            coef_field = coarsen(coef_field)
        coupling = 0.25 ** grid_level
        diagonals.append(coef_field + 6.0 * coupling)
        couplings.append(coupling)

    def operate(field, grid_level):
        return diagonals[grid_level] * field - couplings[grid_level] * neighbours(jnp.pad(field, 1))

    def jacobi_sweep(field, rhs_field, grid_level):
        return field + damping * (rhs_field - operate(field, grid_level)) / diagonals[grid_level]

    def vcycle(rhs_field, grid_level):
        field = damping * rhs_field / diagonals[grid_level]
        if grid_level == LEVELS:
            for sweep_index in range(COARSE_SWEEPS - 1):
                field = jacobi_sweep(field, rhs_field, grid_level)
            return field
        field = jacobi_sweep(field, rhs_field, grid_level)
        remainder = rhs_field - operate(field, grid_level)
        field = field + refine(vcycle(coarsen(remainder), grid_level + 1))
        field = jacobi_sweep(field, rhs_field, grid_level)
        return jacobi_sweep(field, rhs_field, grid_level)

    def solve_one(sign_bits):
        right_side = 2.0 * sign_bits.astype(jnp.float32) - 1.0
        solution = jnp.zeros_like(right_side)
        residual = right_side
        precond = vcycle(residual, 0)
        precond_dot = jnp.sum(residual * precond)
        search = precond
        for iteration in range(ITERS):
            operated = operate(search, 0)
            step_size = precond_dot / jnp.sum(search * operated)
            solution = solution + step_size * search
            residual = residual - step_size * operated
            if iteration + 1 < ITERS:
                precond = vcycle(residual, 0)
                next_dot = jnp.sum(residual * precond)
                search = precond + next_dot / precond_dot * search
                precond_dot = next_dot
        return (solution, jnp.sum(residual * residual))
    solution, squares = lax.map(solve_one, probe_bits)
    cell_total = probe_bits.shape[1] * probe_bits.shape[2] * probe_bits.shape[3]
    return (solution, jnp.sqrt(squares / cell_total))
```

```python
import functools
import math

import jax
import jax.numpy as jnp
from jax import lax
from jax.experimental import pallas as pl
from jax.experimental.pallas import tpu as pltpu
from jax.sharding import PartitionSpec as P

LEVELS = 3
COARSE_SWEEPS = 8
DAMP = 0.8
LANES = 128
F32 = jnp.float32
MESH = pl.DeviceIdType.MESH
AXES = ("gx", "gz", "gy")


def dot(a, b):
    return jnp.dot(a, b, precision=lax.Precision.HIGHEST, preferred_element_type=F32)


def body(cfg, kappa, bits, x_out, rel_out, *scr):
    probes, sizes, counts, reach, width = cfg
    nx, nz, ny = counts["gx"], counts["gz"], counts["gy"]
    total = nx * nz * ny
    (v0, b0, r0, p0, q0, d0, w0, v1, b1, d1, w1,
     xr0, zs0, zr0, ys0, yr0, xr1, zs1, zr1, ys1, yr1, ss, rs,
     tmp, gsend, gk, gr, gss, gks, grs, v2, b2, k2, w2, b3, d2, k3, e3,
     asend, arecv, ass, ars) = scr
    xr, zs, zr, ys, yr = (xr0, xr1), (zs0, zs1), (zr0, zr1), (ys0, ys1), (yr0, yr1)
    me = {a: lax.axis_index(a) for a in AXES}
    coup = [0.25**l for l in range(LEVELS + 1)]

    def iota(shape, dim):
        return lax.broadcasted_iota(jnp.int32, shape, dim)

    def zero(ref):
        ref[...] = jnp.zeros(ref.shape, F32)

    ri, ci = iota((LANES, LANES), 0), iota((LANES, LANES), 1)
    pool_m = jnp.where(ri // 2 == ci, 0.125, 0.0).astype(F32)
    spread_m = jnp.where(ci // 2 == ri, 1.0, 0.0).astype(F32)
    y2 = sizes[2][2]
    own_m = jnp.where((ci // 2 + reach * y2 == ri) & (ci < 2 * y2), 1.0, 0.0).astype(F32)

    def pool(f):
        cx, cz, _ = f.shape
        s = f.reshape(cx // 2, 2, cz, LANES)
        s = (s[:, 0] + s[:, 1]).reshape(cx // 2 * cz, LANES)
        rows = cx // 2 * cz
        tmp[pl.ds(0, rows), :] = s
        h = tmp[pl.ds(0, rows // 2, stride=2), :] + tmp[pl.ds(1, rows // 2, stride=2), :]
        return dot(h, pool_m)

    def spread(e, cx, cz, mat):
        rows = cx * cz
        f = dot(e, mat)
        tmp[pl.ds(0, rows, stride=2), :] = f
        tmp[pl.ds(1, rows, stride=2), :] = f
        g = tmp[pl.ds(0, 2 * rows), :].reshape(cx, 1, 2 * cz, LANES)
        return jnp.broadcast_to(g, (cx, 2, 2 * cz, LANES)).reshape(2 * cx, 2 * cz, LANES)

    def face_copies(level, par, field):
        X = sizes[level][0]
        out = []
        for ai, axis in enumerate(AXES):
            for side in (0, 1):
                if ai == 0:
                    src = field.at[:, 0 if side == 0 else X - 1]
                    dst = xr[level].at[par, 1 - side]
                elif ai == 1:
                    src, dst = zs[level].at[par, side], zr[level].at[par, 1 - side]
                else:
                    src, dst = ys[level].at[par, side], yr[level].at[par, 1 - side]
                step = -1 if side == 0 else 1
                ok = me[axis] > 0 if side == 0 else me[axis] < counts[axis] - 1

                def make(src=src, dst=dst, ai=ai, side=side, axis=axis, step=step, flip=False):
                    return pltpu.make_async_remote_copy(
                        src_ref=src, dst_ref=dst,
                        send_sem=ss.at[level, par, ai, side],
                        recv_sem=rs.at[level, par, ai, side if flip else 1 - side],
                        device_id={axis: me[axis] + step}, device_id_type=MESH)

                out.append((ok, make))
        return out

    def start(level, par, field):
        for ok, make in face_copies(level, par, field):
            @pl.when(ok)
            def _(make=make):
                make().start()

    def finish(level, par, field):
        for ok, make in face_copies(level, par, field):
            @pl.when(ok)
            def _(make=make):
                make(flip=True).wait_recv()
                make().wait_send()

    def pack(level, par, v, p):
        X, Z, Y = sizes[level]
        zs[level][par, 0, p] = v[:, 0:1, :]
        zs[level][par, 1, p] = v[:, Z - 1 : Z, :]
        lane = iota((Z, LANES), 1)
        lo = v[0]
        hi = pltpu.roll(v[0], (LANES - (Y - 1)) % LANES, 1)
        for x in range(1, X):
            lo = jnp.where(lane == x, pltpu.roll(v[x], x, 1), lo)
            hi = jnp.where(lane == x, pltpu.roll(v[x], (x - (Y - 1)) % LANES, 1), hi)
        mine = (lane >= p * X) & (lane < p * X + X)
        ys[level][par, 0] = jnp.where(mine, pltpu.roll(lo, p * X, 1), ys[level][par, 0])
        ys[level][par, 1] = jnp.where(mine, pltpu.roll(hi, p * X, 1), ys[level][par, 1])

    def near(level, par, v, p):
        X, Z, Y = sizes[level]
        sub, lane = iota((X, Z, LANES), 1), iota((X, Z, LANES), 2)
        n = jnp.concatenate([xr[level][par, 0, p][None], v[:-1]], 0)
        n = n + jnp.concatenate([v[1:], xr[level][par, 1, p][None]], 0)
        n = n + jnp.where(sub == 0, zr[level][par, 0, p], pltpu.roll(v, 1, 1))
        n = n + jnp.where(sub == Z - 1, zr[level][par, 1, p], pltpu.roll(v, Z - 1, 1))
        back = lax.rem(LANES - p * X, LANES)
        lo = pltpu.roll(yr[level][par, 0], back, 1)
        hi = pltpu.roll(yr[level][par, 1], back, 1)
        los = jnp.stack([pltpu.roll(lo, (LANES - x) % LANES, 1) for x in range(X)], 0)
        his = jnp.stack([pltpu.roll(hi, (Y - 1 - x) % LANES, 1) for x in range(X)], 0)
        n = n + jnp.where(lane == 0, los, pltpu.roll(v, 1, 2))
        n = n + jnp.where(lane == Y - 1, his, pltpu.roll(v, LANES - 1, 2))
        return n

    def flat_near(v, Y):
        X, Z, _ = v.shape
        sub, lane = iota(v.shape, 1), iota(v.shape, 2)
        none = jnp.zeros((1, Z, LANES), F32)
        n = jnp.concatenate([none, v[:-1]], 0) + jnp.concatenate([v[1:], none], 0)
        n = n + jnp.where(sub == 0, 0.0, pltpu.roll(v, 1, 1))
        n = n + jnp.where(sub == Z - 1, 0.0, pltpu.roll(v, Z - 1, 1))
        n = n + jnp.where(lane == 0, 0.0, pltpu.roll(v, 1, 2))
        n = n + jnp.where(lane >= Y - 1, 0.0, pltpu.roll(v, LANES - 1, 2))
        return n

    def per_probe(fn):
        def step(p, c):
            fn(p)
            return c
        lax.fori_loop(0, probes, step, 0)

    steps = [0, 0]

    def exchange(level, field):
        par = steps[level] % 2
        steps[level] += 1
        start(level, par, field)
        finish(level, par, field)
        return par

    Xc, Zc, Yc = sizes[2]
    rows2 = Xc * Zc

    def gather_copies(dst_ref, sems, which):
        out = []
        for a in range(nx):
            for c in range(nz):
                for o in range(width):
                    if (a, c, o) == (0, 0, reach):
                        continue
                    tx, tz = lax.rem(me["gx"] + a, nx), lax.rem(me["gz"] + c, nz)
                    ty = me["gy"] + (reach - o)
                    slot = (me["gx"] * nz + me["gz"]) * width + o
                    fx, fz = lax.rem(me["gx"] + nx - a, nx), lax.rem(me["gz"] + nz - c, nz)
                    fslot = (fx * nz + fz) * width + o
                    fy = me["gy"] + (o - reach)
                    sidx = (a * nz + c) * width + o

                    def make(tx=tx, tz=tz, ty=ty, slot=slot, sidx=sidx):
                        return pltpu.make_async_remote_copy(
                            src_ref=gsend.at[which], dst_ref=dst_ref.at[slot],
                            send_sem=gss.at[which, sidx], recv_sem=sems.at[slot],
                            device_id={"gx": tx, "gz": tz, "gy": ty}, device_id_type=MESH)

                    def take(tx=tx, tz=tz, ty=ty, fslot=fslot, sidx=sidx):
                        return pltpu.make_async_remote_copy(
                            src_ref=gsend.at[which], dst_ref=dst_ref.at[fslot],
                            send_sem=gss.at[which, sidx], recv_sem=sems.at[fslot],
                            device_id={"gx": tx, "gz": tz, "gy": ty}, device_id_type=MESH)

                    out.append(((ty >= 0) & (ty < ny), make, (fy >= 0) & (fy < ny), take))
        return out

    def gather_start(dst_ref, sems, which):
        for ok, make, _, _ in gather_copies(dst_ref, sems, which):
            @pl.when(ok)
            def _(make=make):
                make().start()
        dst_ref[(me["gx"] * nz + me["gz"]) * width + reach] = gsend[which]

    def gather_finish(dst_ref, sems, which):
        for ok, make, okr, take in gather_copies(dst_ref, sems, which):
            @pl.when(okr)
            def _(take=take):
                take().wait_recv()

            @pl.when(ok)
            def _(make=make):
                make().wait_send()

    def gather_clear(dst_ref):
        for o in range(width):
            fy = me["gy"] + (o - reach)

            @pl.when((fy < 0) | (fy >= ny))
            def _(o=o):
                for s in range(nx * nz):
                    dst_ref[s * width + o] = jnp.zeros((rows2, LANES), F32)

    def unpack(src_ref, out_ref, lead):
        lane = iota((rows2, LANES), 1)
        for sx in range(nx):
            for sz in range(nz):
                tiles = [src_ref[(sx * nz + sz) * width + o] for o in range(width)]
                for p in range(lead):
                    t = jnp.zeros((rows2, LANES), F32)
                    for o in range(width):
                        t = jnp.where(lane // Yc == o, pltpu.roll(tiles[o], ((o - p) * Yc) % LANES, 1), t)
                    for x in range(Xc):
                        out_ref[p, sx * Xc + x, pl.ds(sz * Zc, Zc), :] = t[x * Zc : (x + 1) * Zc]

    def slot_of(x, z, y):
        return (x * nz + z) * ny + y

    def reduce_copies(which, mine_slot):
        out = []
        for a in range(nx):
            for c in range(nz):
                for o in range(ny):
                    if (a, c, o) == (0, 0, 0):
                        continue
                    t = {"gx": lax.rem(me["gx"] + a, nx), "gz": lax.rem(me["gz"] + c, nz),
                         "gy": lax.rem(me["gy"] + o, ny)}
                    f = slot_of(lax.rem(me["gx"] + nx - a, nx), lax.rem(me["gz"] + nz - c, nz),
                                lax.rem(me["gy"] + ny - o, ny))
                    slot = f if not mine_slot else slot_of(me["gx"], me["gz"], me["gy"])
                    out.append(pltpu.make_async_remote_copy(
                        src_ref=asend.at[which], dst_ref=arecv.at[which, slot],
                        send_sem=ass.at[which, slot_of(a, c, o)], recv_sem=ars.at[which, slot],
                        device_id=t, device_id_type=MESH))
        return out

    def reduce_start(which, row):
        asend[which] = row
        for cp in reduce_copies(which, True):
            cp.start()
        arecv[which, slot_of(me["gx"], me["gz"], me["gy"])] = row

    def reduce_finish(which):
        for cp in reduce_copies(which, False):
            cp.wait_recv()
            cp.wait_send()
        return jnp.sum(arecv[which], axis=0)

    lane1 = iota((1, LANES), 1)

    def whole(f):
        s = jnp.sum(f, axis=0)
        return jnp.sum(jnp.sum(s, axis=0, keepdims=True), axis=1, keepdims=True)

    def put(row, q, p, f):
        return jnp.where(lane1 == q * probes + p, whole(f), row)

    def get(row, q, p):
        return jnp.sum(jnp.where(lane1 == q * probes + p, row, 0.0), axis=1, keepdims=True)

    for level in (0, 1):
        for ai, axis in enumerate(AXES):
            for side in (0, 1):
                @pl.when(me[axis] == (0 if side == 0 else counts[axis] - 1))
                def _(level=level, ai=ai, side=side):
                    ref = (xr, zr, yr)[ai][level]
                    for par in (0, 1):
                        ref[par, side] = jnp.zeros(ref.shape[2:], F32)
        zero(ys[level])
    gather_clear(gk)
    for i in (0, 1):
        gather_clear(gr.at[i])

    X0, Z0, Y0 = sizes[0]
    X1, Z1, Y1 = sizes[1]
    k0 = kappa[...]
    d0[...] = k0 + 6.0
    w0[...] = DAMP / d0[...]
    k1 = pool(k0).reshape(X1, Z1, LANES)
    lv1 = iota((X1, Z1, LANES), 2) < Y1
    dd1 = k1 + 6.0 * coup[1]
    d1[...] = dd1
    w1[...] = jnp.where(lv1, DAMP / dd1, 0.0)
    gsend[2] = pool(k1)
    gather_start(gk, gks, 2)

    def first(rhs):
        par = steps[0] % 2

        def fn(p):
            v = w0[...] * rhs[p]
            v0[p] = v
            pack(0, par, v, p)
        return fn

    XG, ZG = nx * Xc, nz * Zc
    WY = width * Yc

    def coefs2():
        gather_finish(gk, gks, 2)
        unpack(gk, k2, 1)
        kk = k2[0]
        lane = iota(kk.shape, 2)
        gy0 = lane + (me["gy"] - reach) * Yc
        ok = (lane < WY) & (gy0 >= 0) & (gy0 < ny * Yc)
        dd = kk + 6.0 * coup[2]
        d2[...] = dd
        w2[...] = jnp.where(ok, DAMP / dd, 0.0)
        c3 = pool(kk).reshape(XG // 2, ZG // 2, LANES)
        lane = iota(c3.shape, 2)
        gy0 = lane + (me["gy"] - reach) * (Yc // 2)
        ok = (lane < WY // 2) & (gy0 >= 0) & (gy0 < ny * (Yc // 2))
        k3[...] = jnp.where(ok, DAMP / (c3 + 6.0 * coup[3]), 0.0)

    def coarse_part(which):
        src = gr.at[which]
        unpack(src, b2, probes)

        def fn(p):
            b = b2[p]
            w = w2[...]
            v = w * b
            v = (1.0 - DAMP) * v + w * (b + coup[2] * flat_near(v, WY))
            r = b - d2[...] * v + coup[2] * flat_near(v, WY)
            r = jnp.where(w > 0.0, r, 0.0)
            c = pool(r).reshape(XG // 2, ZG // 2, LANES)
            w3 = k3[...]
            u = w3 * c
            for _ in range(COARSE_SWEEPS - 1):
                u = (1.0 - DAMP) * u + w3 * (c + coup[3] * flat_near(u, WY // 2))
            e = spread(u.reshape(XG // 2 * (ZG // 2), LANES), XG // 2, ZG // 2, spread_m)
            v = v + jnp.where(w > 0.0, e, 0.0)
            for _ in range(2):
                v = (1.0 - DAMP) * v + w * (b + coup[2] * flat_near(v, WY))
            v2[p] = v
        per_probe(fn)

    def sweep(level, rhs, field, more=True):
        par = exchange(level, field)
        d, w = (d0, d1)[level], (w0, w1)[level]
        nxt = steps[level] % 2

        def fn(p):
            v = field[p]
            v = (1.0 - DAMP) * v + w[...] * (rhs[p] + coup[level] * near(level, par, v, p))
            field[p] = v
            if more:
                pack(level, nxt, v, p)
        per_probe(fn)

    def vcycle(rhs, which):
        per_probe(first(rhs))
        sweep(0, rhs, v0)
        par = exchange(0, v0)
        par1 = steps[1] % 2

        def down(p, par=par):
            v = v0[p]
            r = rhs[p] - d0[...] * v + near(0, par, v, p)
            b = pool(r).reshape(X1, Z1, LANES)
            b1[p] = b
            v = w1[...] * b
            v1[p] = v
            pack(1, par1, v, p)
        per_probe(down)
        sweep(1, b1, v1)
        par = exchange(1, v1)
        gsend[which] = jnp.zeros((rows2, LANES), F32)

        def down1(p, par=par):
            v = v1[p]
            r = b1[p] - d1[...] * v + coup[1] * near(1, par, v, p)
            r = jnp.where(lv1, r, 0.0)
            gsend[which] = gsend[which] + pltpu.roll(pool(r), p * Yc, 1)
        per_probe(down1)
        gather_start(gr.at[which], grs.at[which], which)
        if which == 0:
            coefs2()
        gather_finish(gr.at[which], grs.at[which], which)
        coarse_part(which)
        nxt = steps[1] % 2

        def up1(p):
            for x in range(Xc):
                e3[pl.ds(x * Zc, Zc), :] = v2[p, me["gx"] * Xc + x, pl.ds(me["gz"] * Zc, Zc), :]
            v = v1[p] + spread(e3[...], Xc, Zc, own_m)
            v1[p] = v
            pack(1, nxt, v, p)
        per_probe(up1)
        sweep(1, b1, v1)
        sweep(1, b1, v1, more=False)
        nxt0 = steps[0] % 2

        def up0(p):
            v = v0[p] + spread(v1[p].reshape(X1 * Z1, LANES), X1, Z1, spread_m)
            v0[p] = v
            pack(0, nxt0, v, p)
        per_probe(up0)
        sweep(0, rhs, v0)
        sweep(0, rhs, v0)

    def begin(p):
        r0[p] = 2.0 * bits[p].astype(F32) - 1.0
    per_probe(begin)
    vcycle(r0, 0)
    par = exchange(0, v0)

    def image(p, row, par=par):
        v = v0[p]
        q = d0[...] * v - near(0, par, v, p)
        p0[p] = v
        q0[p] = q
        row = put(row, 0, p, r0[p] * v)
        return put(row, 1, p, v * q)
    row = lax.fori_loop(0, probes, image, jnp.zeros((1, LANES), F32))
    reduce_start(0, row)
    vcycle(q0, 1)
    sums0 = reduce_finish(0)
    nxt = steps[0] % 2

    def direction(p):
        a = get(sums0, 0, p) / get(sums0, 1, p)
        v = p0[p] - a * v0[p]
        v0[p] = v
        r0[p] = r0[p] - a * q0[p]
        pack(0, nxt, v, p)
    per_probe(direction)
    par = exchange(0, v0)

    def image2(p, row, par=par):
        v = v0[p]
        t = d0[...] * v - near(0, par, v, p)
        b0[p] = t
        row = put(row, 0, p, r0[p] * v)
        row = put(row, 1, p, v * t)
        return put(row, 2, p, v * q0[p])
    row = lax.fori_loop(0, probes, image2, jnp.zeros((1, LANES), F32))
    reduce_start(1, row)
    sums1 = reduce_finish(1)

    def final(p, row):
        rz0, pq0 = get(sums0, 0, p), get(sums0, 1, p)
        rz1, pt, pq = get(sums1, 0, p), get(sums1, 1, p), get(sums1, 2, p)
        a0 = rz0 / pq0
        beta = rz1 / rz0
        a1 = rz1 / (pt + 2.0 * beta * pq + beta * beta * pq0)
        x_out[p] = a0 * p0[p] + a1 * (v0[p] + beta * p0[p])
        r = r0[p] - a1 * (b0[p] + beta * q0[p])
        return put(row, 0, p, r * r)
    row = lax.fori_loop(0, probes, final, jnp.zeros((1, LANES), F32))
    reduce_start(2, row)
    cells = float(X0 * Z0 * Y0 * total)
    rel_out[...] = jnp.sqrt(reduce_finish(2) / cells)


def per_device(mesh_counts, kappa_sq, probe_bits):
    probes, X, Z, Y = probe_bits.shape
    sizes = [(X >> l, Z >> l, Y >> l) for l in range(LEVELS + 1)]
    need = 2 * (1 + COARSE_SWEEPS - 1) + 2
    reach = min(math.ceil(need / sizes[2][2]), mesh_counts["gy"] - 1)
    width = 2 * reach + 1
    assert Y <= LANES and width * sizes[2][2] <= LANES and probes * X <= LANES
    assert probes * sizes[2][2] <= LANES
    nx, nz, ny = mesh_counts["gx"], mesh_counts["gz"], mesh_counts["gy"]
    total = nx * nz * ny
    slots = nx * nz * width
    Xc, Zc, Yc = sizes[2]
    XG, ZG = nx * Xc, nz * Zc

    def vm(*shape):
        return pltpu.VMEM(shape, F32)

    def full(level):
        return vm(probes, sizes[level][0], sizes[level][1], LANES)

    def coef(level):
        return vm(sizes[level][0], sizes[level][1], LANES)

    def halo(level):
        x, z, _ = sizes[level]
        return [vm(2, 2, probes, z, LANES), vm(2, 2, probes, x, 1, LANES),
                vm(2, 2, probes, x, 1, LANES), vm(2, 2, z, LANES), vm(2, 2, z, LANES)]

    dma = pltpu.SemaphoreType.DMA
    scratch = [full(0), full(0), full(0), full(0), full(0), coef(0), coef(0),
               full(1), full(1), coef(1), coef(1), *halo(0), *halo(1),
               dma((2, 2, 3, 2)), dma((2, 2, 3, 2)),
               vm(max(X * Z, XG * ZG), LANES), vm(3, Xc * Zc, LANES),
               vm(slots, Xc * Zc, LANES), vm(2, slots, Xc * Zc, LANES),
               dma((3, slots)), dma((slots,)), dma((2, slots)),
               vm(probes, XG, ZG, LANES), vm(probes, XG, ZG, LANES), vm(1, XG, ZG, LANES),
               vm(XG, ZG, LANES), vm(probes, XG // 2, ZG // 2, LANES), vm(XG, ZG, LANES),
               vm(XG // 2, ZG // 2, LANES), vm(Xc * Zc, LANES),
               vm(3, 1, LANES), vm(3, total, 1, LANES), dma((3, total)), dma((3, total))]
    cfg = (probes, sizes, mesh_counts, reach, width)
    field, rel = pl.pallas_call(
        functools.partial(body, cfg),
        out_shape=(jax.ShapeDtypeStruct(probe_bits.shape, F32),
                   jax.ShapeDtypeStruct((1, LANES), F32)),
        in_specs=[pl.BlockSpec(memory_space=pltpu.VMEM)] * 2,
        out_specs=(pl.BlockSpec(memory_space=pltpu.VMEM),) * 2,
        scratch_shapes=scratch,
        compiler_params=pltpu.CompilerParams(has_side_effects=True, vmem_limit_bytes=48 * 2**20),
    )(kappa_sq, probe_bits)
    return field, rel[0, :probes]


def solution(mesh):
    return jax.shard_map(
        functools.partial(per_device, dict(mesh.shape)),
        mesh=mesh,
        in_specs=(P("gx", "gz", "gy"), P(None, "gx", "gz", "gy")),
        out_specs=(P(None, "gx", "gz", "gy"), P()),
        check_vma=False,
    )
```

```python
import functools
import math

import jax
import jax.numpy as jnp
from jax import lax
from jax.experimental import pallas as pl
from jax.experimental.pallas import tpu as pltpu
from jax.sharding import PartitionSpec as P

LEVELS = 3
COARSE_SWEEPS = 8
DAMP = 0.8
LANES = 128
F32 = jnp.float32
MESH = pl.DeviceIdType.MESH
AXES = ("gx", "gz", "gy")


def dot(a, b):
    return jnp.dot(a, b, precision=lax.Precision.HIGHEST, preferred_element_type=F32)


def body(cfg, kappa, bits, x_out, rel_out, *scr):
    probes, sizes, counts, reach, width = cfg
    nx, nz, ny = counts["gx"], counts["gz"], counts["gy"]
    total = nx * nz * ny
    (v0, b0, r0, p0, q0, d0, w0, v1, b1, d1, w1,
     xr0, zs0, zr0, ys0, yr0, ym0, xr1, zs1, zr1, ys1, yr1, ym1, ss, rs,
     tmp, gsend, gk, gr, gss, gks, grs, v2, b2, k2, w2, b3, d2, k3, e3, c3, acc1,
     asend, arecv, ass, ars) = scr
    xr, zs, zr, ys, yr = (xr0, xr1), (zs0, zs1), (zr0, zr1), (ys0, ys1), (yr0, yr1)
    ym, acc = (ym0, ym1), (b0, acc1)
    me = {a: lax.axis_index(a) for a in AXES}
    coup = [0.25**l for l in range(LEVELS + 1)]

    def iota(shape, dim):
        return lax.broadcasted_iota(jnp.int32, shape, dim)

    def zero(ref):
        ref[...] = jnp.zeros(ref.shape, F32)

    ri, ci = iota((LANES, LANES), 0), iota((LANES, LANES), 1)
    pool_m = jnp.where(ri // 2 == ci, 0.125, 0.0).astype(F32)
    spread_m = jnp.where(ci // 2 == ri, 1.0, 0.0).astype(F32)
    y2 = sizes[2][2]
    own_m = jnp.where((ci // 2 + reach * y2 == ri) & (ci < 2 * y2), 1.0, 0.0).astype(F32)

    def pool(f):
        cx, cz, _ = f.shape
        s = f.reshape(cx // 2, 2, cz, LANES)
        s = (s[:, 0] + s[:, 1]).reshape(cx // 2 * cz, LANES)
        rows = cx // 2 * cz
        tmp[pl.ds(0, rows), :] = s
        h = tmp[pl.ds(0, rows // 2, stride=2), :] + tmp[pl.ds(1, rows // 2, stride=2), :]
        return dot(h, pool_m)

    def spread(e, cx, cz, mat):
        rows = cx * cz
        f = dot(e, mat)
        tmp[pl.ds(0, rows, stride=2), :] = f
        tmp[pl.ds(1, rows, stride=2), :] = f
        g = tmp[pl.ds(0, 2 * rows), :].reshape(cx, 1, 2 * cz, LANES)
        return jnp.broadcast_to(g, (cx, 2, 2 * cz, LANES)).reshape(2 * cx, 2 * cz, LANES)

    def face_copies(level, par, field, axes, p=None):
        X = sizes[level][0]
        out = []
        for ai in axes:
            axis = AXES[ai]
            for side in (0, 1):
                if ai == 0:
                    src = field.at[:, 0 if side == 0 else X - 1]
                    dst = xr[level].at[par, 1 - side]
                elif ai == 1:
                    src, dst = zs[level].at[par, side], zr[level].at[par, 1 - side]
                else:
                    src, dst = ys[level].at[par], yr[level].at[par, 1 - side]
                if p is not None:
                    src, dst = src.at[p], dst.at[p]
                step = -1 if side == 0 else 1
                ok = me[axis] > 0 if side == 0 else me[axis] < counts[axis] - 1

                def make(src=src, dst=dst, ai=ai, side=side, axis=axis, step=step, flip=False):
                    return pltpu.make_async_remote_copy(
                        src_ref=src, dst_ref=dst,
                        send_sem=ss.at[level, par, ai, side],
                        recv_sem=rs.at[level, par, ai, side if flip else 1 - side],
                        device_id={axis: me[axis] + step}, device_id_type=MESH)

                out.append((ok, make))
        return out

    def start(level, par, field, axes, p=None):
        for ok, make in face_copies(level, par, field, axes, p):
            @pl.when(ok)
            def _(make=make):
                make().start()

    def finish(level, par, field):
        for ok, make in face_copies(level, par, field, (0, 1, 2)):
            @pl.when(ok)
            def _(make=make):
                make(flip=True).wait_recv()
                make().wait_send()
        X, Z, Y = sizes[level]
        lane = iota((Z, LANES), 1)
        low = lane % 2 == 1 if Y == LANES else lane < probes * X
        ym[level][...] = jnp.where(
            low, pltpu.roll(yr[level][par, 0], LANES - (Y - 1), 1),
            pltpu.roll(yr[level][par, 1], Y - 1, 1))

    def lane_of(level, p, x):
        X, _, Y = sizes[level]
        return 2 * (p * X + x) + 1 if Y == LANES else p * X + x

    def pack(level, par, field, v, p):
        X, Z, Y = sizes[level]
        field[p] = v
        zs[level][par, 0, p] = v[:, 0:1, :]
        zs[level][par, 1, p] = v[:, Z - 1 : Z, :]
        start(level, par, field, (0, 1), p)
        lane = iota((Z, LANES), 1)
        tile = ys[level][par]
        for x in range(X):
            s = lane_of(level, p, x)
            hit = (lane == s) | (lane == lax.rem(s + Y - 1, LANES))
            tile = jnp.where(hit, pltpu.roll(v[x], s, 1), tile)
        ys[level][par] = tile

    def halo(level, par, p):
        X, Z, Y = sizes[level]
        sub, lane = iota((Z, LANES), 0), iota((Z, LANES), 1)
        edge = (lane == 0) | (lane == Y - 1)
        m = ym[level][...]
        planes = []
        for x in range(X):
            back = lax.rem(2 * LANES - lane_of(level, p, x), LANES)
            h = jnp.where(edge, pltpu.roll(m, back, 1), 0.0)
            h = h + jnp.where(sub == 0, zr[level][par, 0, p, x],
                              jnp.where(sub == Z - 1, zr[level][par, 1, p, x], 0.0))
            if x == 0:
                h = h + xr[level][par, 0, p]
            if x == X - 1:
                h = h + xr[level][par, 1, p]
            planes.append(h)
        return jnp.stack(planes, 0)

    def flat_near(v, Y):
        X, Z, _ = v.shape
        sub, lane = iota(v.shape, 1), iota(v.shape, 2)
        none = jnp.zeros((1, Z, LANES), F32)
        n = jnp.concatenate([none, v[:-1]], 0) + jnp.concatenate([v[1:], none], 0)
        n = n + jnp.where(sub == 0, 0.0, pltpu.roll(v, 1, 1))
        n = n + jnp.where(sub == Z - 1, 0.0, pltpu.roll(v, Z - 1, 1))
        n = n + jnp.where(lane == 0, 0.0, pltpu.roll(v, 1, 2))
        n = n + jnp.where(lane >= Y - 1, 0.0, pltpu.roll(v, LANES - 1, 2))
        return n

    def per_probe(fn):
        def step(p, c):
            fn(p)
            return c
        lax.fori_loop(0, probes, step, 0)

    steps = [0, 0]

    def exchange(level, field, inner):
        par = steps[level] % 2
        steps[level] += 1
        start(level, par, field, (2,))

        def fn(p):
            v = field[p]
            acc[level][p] = inner(p, v, flat_near(v, sizes[level][2]))
        per_probe(fn)
        finish(level, par, field)
        return par

    Xc, Zc, Yc = sizes[2]
    rows2 = Xc * Zc

    def gather_copies(dst_ref, sems, which):
        out = []
        for a in range(nx):
            for c in range(nz):
                for o in range(width):
                    if (a, c, o) == (0, 0, reach):
                        continue
                    tx, tz = lax.rem(me["gx"] + a, nx), lax.rem(me["gz"] + c, nz)
                    ty = me["gy"] + (reach - o)
                    slot = (me["gx"] * nz + me["gz"]) * width + o
                    fx, fz = lax.rem(me["gx"] + nx - a, nx), lax.rem(me["gz"] + nz - c, nz)
                    fslot = (fx * nz + fz) * width + o
                    fy = me["gy"] + (o - reach)
                    sidx = (a * nz + c) * width + o

                    def make(tx=tx, tz=tz, ty=ty, slot=slot, sidx=sidx):
                        return pltpu.make_async_remote_copy(
                            src_ref=gsend.at[which], dst_ref=dst_ref.at[slot],
                            send_sem=gss.at[which, sidx], recv_sem=sems.at[slot],
                            device_id={"gx": tx, "gz": tz, "gy": ty}, device_id_type=MESH)

                    def take(tx=tx, tz=tz, ty=ty, fslot=fslot, sidx=sidx):
                        return pltpu.make_async_remote_copy(
                            src_ref=gsend.at[which], dst_ref=dst_ref.at[fslot],
                            send_sem=gss.at[which, sidx], recv_sem=sems.at[fslot],
                            device_id={"gx": tx, "gz": tz, "gy": ty}, device_id_type=MESH)

                    out.append(((ty >= 0) & (ty < ny), make, (fy >= 0) & (fy < ny), take))
        return out

    def gather_start(dst_ref, sems, which):
        for ok, make, _, _ in gather_copies(dst_ref, sems, which):
            @pl.when(ok)
            def _(make=make):
                make().start()
        dst_ref[(me["gx"] * nz + me["gz"]) * width + reach] = gsend[which]

    def gather_finish(dst_ref, sems, which):
        for ok, make, okr, take in gather_copies(dst_ref, sems, which):
            @pl.when(okr)
            def _(take=take):
                take().wait_recv()

            @pl.when(ok)
            def _(make=make):
                make().wait_send()

    def gather_clear(dst_ref):
        for o in range(width):
            fy = me["gy"] + (o - reach)

            @pl.when((fy < 0) | (fy >= ny))
            def _(o=o):
                for s in range(nx * nz):
                    dst_ref[s * width + o] = jnp.zeros((rows2, LANES), F32)

    def unpack(src_ref, out_ref, lead):
        lane = iota((rows2, LANES), 1)
        for sx in range(nx):
            for sz in range(nz):
                tiles = [src_ref[(sx * nz + sz) * width + o] for o in range(width)]
                for p in range(lead):
                    t = jnp.zeros((rows2, LANES), F32)
                    for o in range(width):
                        t = jnp.where(lane // Yc == o, pltpu.roll(tiles[o], ((o - p) * Yc) % LANES, 1), t)
                    for x in range(Xc):
                        out_ref[p, sx * Xc + x, pl.ds(sz * Zc, Zc), :] = t[x * Zc : (x + 1) * Zc]

    def slot_of(x, z, y):
        return (x * nz + z) * ny + y

    def reduce_copies(which, mine_slot):
        out = []
        for a in range(nx):
            for c in range(nz):
                for o in range(ny):
                    if (a, c, o) == (0, 0, 0):
                        continue
                    t = {"gx": lax.rem(me["gx"] + a, nx), "gz": lax.rem(me["gz"] + c, nz),
                         "gy": lax.rem(me["gy"] + o, ny)}
                    f = slot_of(lax.rem(me["gx"] + nx - a, nx), lax.rem(me["gz"] + nz - c, nz),
                                lax.rem(me["gy"] + ny - o, ny))
                    slot = f if not mine_slot else slot_of(me["gx"], me["gz"], me["gy"])
                    out.append(pltpu.make_async_remote_copy(
                        src_ref=asend.at[which], dst_ref=arecv.at[which, slot],
                        send_sem=ass.at[which, slot_of(a, c, o)], recv_sem=ars.at[which, slot],
                        device_id=t, device_id_type=MESH))
        return out

    def reduce_start(which, row):
        asend[which] = row
        for cp in reduce_copies(which, True):
            cp.start()
        arecv[which, slot_of(me["gx"], me["gz"], me["gy"])] = row

    def reduce_finish(which):
        for cp in reduce_copies(which, False):
            cp.wait_recv()
            cp.wait_send()
        return jnp.sum(arecv[which], axis=0)

    lane1 = iota((1, LANES), 1)

    def whole(f):
        s = jnp.sum(f, axis=0)
        return jnp.sum(jnp.sum(s, axis=0, keepdims=True), axis=1, keepdims=True)

    def put(row, q, p, f):
        return jnp.where(lane1 == q * probes + p, whole(f), row)

    def get(row, q, p):
        return jnp.sum(jnp.where(lane1 == q * probes + p, row, 0.0), axis=1, keepdims=True)

    for level in (0, 1):
        for ai, axis in enumerate(AXES):
            for side in (0, 1):
                @pl.when(me[axis] == (0 if side == 0 else counts[axis] - 1))
                def _(level=level, ai=ai, side=side):
                    ref = (xr, zr, yr)[ai][level]
                    for par in (0, 1):
                        ref[par, side] = jnp.zeros(ref.shape[2:], F32)
        zero(ys[level])
    gather_clear(gk)
    for i in (0, 1):
        gather_clear(gr.at[i])

    X0, Z0, Y0 = sizes[0]
    X1, Z1, Y1 = sizes[1]
    k0 = kappa[...]
    d0[...] = k0 + 6.0
    w0[...] = DAMP / d0[...]
    k1 = pool(k0).reshape(X1, Z1, LANES)
    lv1 = iota((X1, Z1, LANES), 2) < Y1
    dd1 = k1 + 6.0 * coup[1]
    d1[...] = dd1
    w1[...] = jnp.where(lv1, DAMP / dd1, 0.0)
    gsend[2] = pool(k1)
    gather_start(gk, gks, 2)

    def first(rhs):
        par = steps[0] % 2

        def fn(p):
            pack(0, par, v0, w0[...] * rhs[p], p)
        return fn

    XG, ZG = nx * Xc, nz * Zc
    WY = width * Yc

    def coefs2():
        gather_finish(gk, gks, 2)
        unpack(gk, k2, 1)
        kk = k2[0]
        lane = iota(kk.shape, 2)
        gy0 = lane + (me["gy"] - reach) * Yc
        ok = (lane < WY) & (gy0 >= 0) & (gy0 < ny * Yc)
        dd = kk + 6.0 * coup[2]
        d2[...] = dd
        w2[...] = jnp.where(ok, DAMP / dd, 0.0)
        kc = pool(kk).reshape(XG // 2, ZG // 2, LANES)
        lane = iota(kc.shape, 2)
        gy0 = lane + (me["gy"] - reach) * (Yc // 2)
        ok = (lane < WY // 2) & (gy0 >= 0) & (gy0 < ny * (Yc // 2))
        k3[...] = jnp.where(ok, DAMP / (kc + 6.0 * coup[3]), 0.0)

    def coarse_part(which):
        src = gr.at[which]
        unpack(src, b2, probes)

        def down2(p):
            b = b2[p]
            w = w2[...]
            v = w * b
            v = (1.0 - DAMP) * v + w * (b + coup[2] * flat_near(v, WY))
            v2[p] = v
            r = b - d2[...] * v + coup[2] * flat_near(v, WY)
            r = jnp.where(w > 0.0, r, 0.0)
            c3[p] = pool(r).reshape(XG // 2, ZG // 2, LANES)
        per_probe(down2)
        w3 = k3[...]
        us = [w3 * c3[p] for p in range(probes)]
        for _ in range(COARSE_SWEEPS - 1):
            us = [(1.0 - DAMP) * u + w3 * (c3[p] + coup[3] * flat_near(u, WY // 2))
                  for p, u in enumerate(us)]
        for p in range(probes):
            c3[p] = us[p]

        def up2(p):
            b = b2[p]
            w = w2[...]
            e = spread(c3[p].reshape(XG // 2 * (ZG // 2), LANES), XG // 2, ZG // 2, spread_m)
            v = v2[p] + jnp.where(w > 0.0, e, 0.0)
            for _ in range(2):
                v = (1.0 - DAMP) * v + w * (b + coup[2] * flat_near(v, WY))
            v2[p] = v
        per_probe(up2)

    def sweep(level, rhs, field, more=True):
        d, w = (d0, d1)[level], (w0, w1)[level]

        def inner(p, v, n):
            return (1.0 - DAMP) * v + w[...] * (rhs[p] + coup[level] * n)
        par = exchange(level, field, inner)
        nxt = steps[level] % 2

        def fn(p):
            v = acc[level][p] + w[...] * (coup[level] * halo(level, par, p))
            if more:
                pack(level, nxt, field, v, p)
            else:
                field[p] = v
        per_probe(fn)

    def vcycle(rhs, which):
        per_probe(first(rhs))
        sweep(0, rhs, v0)
        par = exchange(0, v0, lambda p, v, n: rhs[p] - d0[...] * v + n)
        par1 = steps[1] % 2

        def down(p, par=par):
            r = acc[0][p] + halo(0, par, p)
            b = pool(r).reshape(X1, Z1, LANES)
            b1[p] = b
            pack(1, par1, v1, w1[...] * b, p)
        per_probe(down)
        sweep(1, b1, v1)
        par = exchange(1, v1, lambda p, v, n: b1[p] - d1[...] * v + coup[1] * n)
        gsend[which] = jnp.zeros((rows2, LANES), F32)

        def down1(p, par=par):
            r = acc[1][p] + coup[1] * halo(1, par, p)
            r = jnp.where(lv1, r, 0.0)
            gsend[which] = gsend[which] + pltpu.roll(pool(r), p * Yc, 1)
        per_probe(down1)
        gather_start(gr.at[which], grs.at[which], which)
        if which == 0:
            coefs2()
        gather_finish(gr.at[which], grs.at[which], which)
        coarse_part(which)
        nxt = steps[1] % 2

        def up1(p):
            for x in range(Xc):
                e3[pl.ds(x * Zc, Zc), :] = v2[p, me["gx"] * Xc + x, pl.ds(me["gz"] * Zc, Zc), :]
            v = v1[p] + spread(e3[...], Xc, Zc, own_m)
            pack(1, nxt, v1, v, p)
        per_probe(up1)
        sweep(1, b1, v1)
        sweep(1, b1, v1, more=False)
        nxt0 = steps[0] % 2

        def up0(p):
            v = v0[p] + spread(v1[p].reshape(X1 * Z1, LANES), X1, Z1, spread_m)
            pack(0, nxt0, v0, v, p)
        per_probe(up0)
        sweep(0, rhs, v0)
        sweep(0, rhs, v0, more=which == 0)

    def begin(p):
        r0[p] = 2.0 * bits[p].astype(F32) - 1.0
    per_probe(begin)
    vcycle(r0, 0)
    par = exchange(0, v0, lambda p, v, n: d0[...] * v - n)

    def image(p, row, par=par):
        v = v0[p]
        q = acc[0][p] - halo(0, par, p)
        p0[p] = v
        q0[p] = q
        row = put(row, 0, p, r0[p] * v)
        return put(row, 1, p, v * q)
    row = lax.fori_loop(0, probes, image, jnp.zeros((1, LANES), F32))
    reduce_start(0, row)
    vcycle(q0, 1)
    sums0 = reduce_finish(0)
    nxt = steps[0] % 2

    def direction(p):
        a = get(sums0, 0, p) / get(sums0, 1, p)
        v = p0[p] - a * v0[p]
        r0[p] = r0[p] - a * q0[p]
        pack(0, nxt, v0, v, p)
    per_probe(direction)
    par = exchange(0, v0, lambda p, v, n: d0[...] * v - n)

    def image2(p, row, par=par):
        v = v0[p]
        t = acc[0][p] - halo(0, par, p)
        b0[p] = t
        row = put(row, 0, p, r0[p] * v)
        row = put(row, 1, p, v * t)
        return put(row, 2, p, v * q0[p])
    row = lax.fori_loop(0, probes, image2, jnp.zeros((1, LANES), F32))
    reduce_start(1, row)
    sums1 = reduce_finish(1)

    def final(p, row):
        rz0, pq0 = get(sums0, 0, p), get(sums0, 1, p)
        rz1, pt, pq = get(sums1, 0, p), get(sums1, 1, p), get(sums1, 2, p)
        a0 = rz0 / pq0
        beta = rz1 / rz0
        a1 = rz1 / (pt + 2.0 * beta * pq + beta * beta * pq0)
        x_out[p] = a0 * p0[p] + a1 * (v0[p] + beta * p0[p])
        r = r0[p] - a1 * (b0[p] + beta * q0[p])
        return put(row, 0, p, r * r)
    row = lax.fori_loop(0, probes, final, jnp.zeros((1, LANES), F32))
    reduce_start(2, row)
    cells = float(X0 * Z0 * Y0 * total)
    rel_out[...] = jnp.sqrt(reduce_finish(2) / cells)


def per_device(mesh_counts, kappa_sq, probe_bits):
    probes, X, Z, Y = probe_bits.shape
    sizes = [(X >> l, Z >> l, Y >> l) for l in range(LEVELS + 1)]
    need = 2 * (1 + COARSE_SWEEPS - 1) + 2
    reach = min(math.ceil(need / sizes[2][2]), mesh_counts["gy"] - 1)
    width = 2 * reach + 1
    assert Y <= LANES and width * sizes[2][2] <= LANES and probes * X <= LANES
    assert probes * sizes[2][2] <= LANES
    nx, nz, ny = mesh_counts["gx"], mesh_counts["gz"], mesh_counts["gy"]
    total = nx * nz * ny
    slots = nx * nz * width
    Xc, Zc, Yc = sizes[2]
    XG, ZG = nx * Xc, nz * Zc

    def vm(*shape):
        return pltpu.VMEM(shape, F32)

    def full(level):
        return vm(probes, sizes[level][0], sizes[level][1], LANES)

    def coef(level):
        return vm(sizes[level][0], sizes[level][1], LANES)

    def halo(level):
        x, z, _ = sizes[level]
        return [vm(2, 2, probes, z, LANES), vm(2, 2, probes, x, 1, LANES),
                vm(2, 2, probes, x, 1, LANES), vm(2, z, LANES), vm(2, 2, z, LANES), vm(z, LANES)]

    dma = pltpu.SemaphoreType.DMA
    scratch = [full(0), full(0), full(0), full(0), full(0), coef(0), coef(0),
               full(1), full(1), coef(1), coef(1), *halo(0), *halo(1),
               dma((2, 2, 3, 2)), dma((2, 2, 3, 2)),
               vm(max(X * Z, XG * ZG), LANES), vm(3, Xc * Zc, LANES),
               vm(slots, Xc * Zc, LANES), vm(2, slots, Xc * Zc, LANES),
               dma((3, slots)), dma((slots,)), dma((2, slots)),
               vm(probes, XG, ZG, LANES), vm(probes, XG, ZG, LANES), vm(1, XG, ZG, LANES),
               vm(XG, ZG, LANES), vm(probes, XG // 2, ZG // 2, LANES), vm(XG, ZG, LANES),
               vm(XG // 2, ZG // 2, LANES), vm(Xc * Zc, LANES),
               vm(probes, XG // 2, ZG // 2, LANES), full(1),
               vm(3, 1, LANES), vm(3, total, 1, LANES), dma((3, total)), dma((3, total))]
    cfg = (probes, sizes, mesh_counts, reach, width)
    field, rel = pl.pallas_call(
        functools.partial(body, cfg),
        out_shape=(jax.ShapeDtypeStruct(probe_bits.shape, F32),
                   jax.ShapeDtypeStruct((1, LANES), F32)),
        in_specs=[pl.BlockSpec(memory_space=pltpu.VMEM)] * 2,
        out_specs=(pl.BlockSpec(memory_space=pltpu.VMEM),) * 2,
        scratch_shapes=scratch,
        compiler_params=pltpu.CompilerParams(has_side_effects=True, vmem_limit_bytes=48 * 2**20),
    )(kappa_sq, probe_bits)
    return field, rel[0, :probes]


def solution(mesh):
    return jax.shard_map(
        functools.partial(per_device, dict(mesh.shape)),
        mesh=mesh,
        in_specs=(P("gx", "gz", "gy"), P(None, "gx", "gz", "gy")),
        out_specs=(P(None, "gx", "gz", "gy"), P()),
        check_vma=False,
    )
```

```python
import functools
import math

import jax
import jax.numpy as jnp
from jax import lax
from jax.experimental import pallas as pl
from jax.experimental.pallas import tpu as pltpu
from jax.sharding import PartitionSpec as P

LEVELS = 3
COARSE_SWEEPS = 8
DAMP = 0.8
LANES = 128
F32 = jnp.float32
MESH = pl.DeviceIdType.MESH
AXES = ("gx", "gz", "gy")


def dot(a, b):
    return jnp.dot(a, b, precision=lax.Precision.HIGHEST, preferred_element_type=F32)


def body(cfg, kappa, bits, x_out, rel_out, *scr):
    probes, sizes, counts, reach, width = cfg
    nx, nz, ny = counts["gx"], counts["gz"], counts["gy"]
    total = nx * nz * ny
    (v0, b0, r0, p0, q0, d0, w0, v1, b1, d1, w1,
     xr0, zs0, zr0, ys0, yr0, ym0, xr1, zs1, zr1, ys1, yr1, ym1, ss, rs,
     tmp, gsend, gk, gr, gss, gks, grs, v2, b2, k2, w2, b3, d2, k3, e3, c3, acc1,
     asend, arecv, ass, ars) = scr
    xr, zs, zr, ys, yr = (xr0, xr1), (zs0, zs1), (zr0, zr1), (ys0, ys1), (yr0, yr1)
    ym, acc = (ym0, ym1), (b0, acc1)
    me = {a: lax.axis_index(a) for a in AXES}
    coup = [0.25**l for l in range(LEVELS + 1)]

    def iota(shape, dim):
        return lax.broadcasted_iota(jnp.int32, shape, dim)

    def zero(ref):
        ref[...] = jnp.zeros(ref.shape, F32)

    ri, ci = iota((LANES, LANES), 0), iota((LANES, LANES), 1)
    pool_m = jnp.where(ri // 2 == ci, 0.125, 0.0).astype(F32)
    spread_m = jnp.where(ci // 2 == ri, 1.0, 0.0).astype(F32)
    y2 = sizes[2][2]
    own_m = jnp.where((ci // 2 + reach * y2 == ri) & (ci < 2 * y2), 1.0, 0.0).astype(F32)

    def pool(f, k=0):
        cx, cz, _ = f.shape
        s = f.reshape(cx // 2, 2, cz, LANES)
        s = (s[:, 0] + s[:, 1]).reshape(cx // 2 * cz, LANES)
        rows = cx // 2 * cz
        t = tmp.at[k]
        t[pl.ds(0, rows), :] = s
        h = t[pl.ds(0, rows // 2, stride=2), :] + t[pl.ds(1, rows // 2, stride=2), :]
        return dot(h, pool_m)

    def spread(e, cx, cz, mat, k=0):
        rows = cx * cz
        f = dot(e, mat)
        t = tmp.at[k]
        t[pl.ds(0, rows, stride=2), :] = f
        t[pl.ds(1, rows, stride=2), :] = f
        g = t[pl.ds(0, 2 * rows), :].reshape(cx, 1, 2 * cz, LANES)
        return jnp.broadcast_to(g, (cx, 2, 2 * cz, LANES)).reshape(2 * cx, 2 * cz, LANES)

    def face_copies(level, par, field, axes, p=None):
        X = sizes[level][0]
        out = []
        for ai in axes:
            axis = AXES[ai]
            for side in (0, 1):
                if ai == 0:
                    src = field.at[:, 0 if side == 0 else X - 1]
                    dst = xr[level].at[par, 1 - side]
                elif ai == 1:
                    src, dst = zs[level].at[par, side], zr[level].at[par, 1 - side]
                else:
                    src, dst = ys[level].at[par], yr[level].at[par, 1 - side]
                if p is not None:
                    src, dst = src.at[p], dst.at[p]
                step = -1 if side == 0 else 1
                ok = me[axis] > 0 if side == 0 else me[axis] < counts[axis] - 1

                def make(src=src, dst=dst, ai=ai, side=side, axis=axis, step=step, flip=False):
                    return pltpu.make_async_remote_copy(
                        src_ref=src, dst_ref=dst,
                        send_sem=ss.at[level, par, ai, side],
                        recv_sem=rs.at[level, par, ai, side if flip else 1 - side],
                        device_id={axis: me[axis] + step}, device_id_type=MESH)

                out.append((ok, make))
        return out

    def start(level, par, field, axes, p=None):
        for ok, make in face_copies(level, par, field, axes, p):
            @pl.when(ok)
            def _(make=make):
                make().start()

    def finish(level, par, field):
        for ok, make in face_copies(level, par, field, (0, 1, 2)):
            @pl.when(ok)
            def _(make=make):
                make(flip=True).wait_recv()
                make().wait_send()
        X, Z, Y = sizes[level]
        lane = iota((Z, LANES), 1)
        low = lane % 2 == 1 if Y == LANES else lane < probes * X
        ym[level][...] = jnp.where(
            low, pltpu.roll(yr[level][par, 0], LANES - (Y - 1), 1),
            pltpu.roll(yr[level][par, 1], Y - 1, 1))

    def lane_of(level, p, x):
        X, _, Y = sizes[level]
        return 2 * (p * X + x) + 1 if Y == LANES else p * X + x

    def pack(level, par, field, v, p, send=True):
        X, Z, Y = sizes[level]
        field[p] = v
        zs[level][par, 0, p] = v[:, 0:1, :]
        zs[level][par, 1, p] = v[:, Z - 1 : Z, :]
        lane = iota((Z, LANES), 1)
        tile = ys[level][par]
        for x in range(X):
            s = lane_of(level, p, x)
            hit = (lane == s) | (lane == (s + Y - 1) % LANES)
            tile = jnp.where(hit, pltpu.roll(v[x], s, 1), tile)
        ys[level][par] = tile
        if send:
            start(level, par, field, (0, 1), p)

    def halo(level, par, p):
        X, Z, Y = sizes[level]
        sub, lane = iota((Z, LANES), 0), iota((Z, LANES), 1)
        edge = (lane == 0) | (lane == Y - 1)
        m = ym[level][...]
        planes = []
        for x in range(X):
            back = (2 * LANES - lane_of(level, p, x)) % LANES
            h = jnp.where(edge, pltpu.roll(m, back, 1), 0.0)
            h = h + jnp.where(sub == 0, zr[level][par, 0, p, x],
                              jnp.where(sub == Z - 1, zr[level][par, 1, p, x], 0.0))
            if x == 0:
                h = h + xr[level][par, 0, p]
            if x == X - 1:
                h = h + xr[level][par, 1, p]
            planes.append(h)
        return jnp.stack(planes, 0)

    def flat_near(v, Y):
        X, Z, _ = v.shape
        sub, lane = iota(v.shape, 1), iota(v.shape, 2)
        none = jnp.zeros((1, Z, LANES), F32)
        n = jnp.concatenate([none, v[:-1]], 0) + jnp.concatenate([v[1:], none], 0)
        n = n + jnp.where(sub == 0, 0.0, pltpu.roll(v, 1, 1))
        n = n + jnp.where(sub == Z - 1, 0.0, pltpu.roll(v, Z - 1, 1))
        n = n + jnp.where(lane == 0, 0.0, pltpu.roll(v, 1, 2))
        n = n + jnp.where(lane >= Y - 1, 0.0, pltpu.roll(v, LANES - 1, 2))
        return n

    def per_probe(fn, unroll=False):
        if unroll:
            for p in range(probes):
                fn(p)
            return

        def step(p, c):
            fn(p)
            return c
        lax.fori_loop(0, probes, step, 0)

    steps = [0, 0]

    def exchange(level, field, inner):
        par = steps[level] % 2
        steps[level] += 1
        start(level, par, field, (2,))

        def fn(p):
            v = field[p]
            acc[level][p] = inner(p, v, flat_near(v, sizes[level][2]))
        per_probe(fn, level == 1)
        finish(level, par, field)
        return par

    Xc, Zc, Yc = sizes[2]
    rows2 = Xc * Zc

    def gather_copies(dst_ref, sems, which):
        out = []
        for a in range(nx):
            for c in range(nz):
                for o in range(width):
                    if (a, c, o) == (0, 0, reach):
                        continue
                    tx, tz = lax.rem(me["gx"] + a, nx), lax.rem(me["gz"] + c, nz)
                    ty = me["gy"] + (reach - o)
                    slot = (me["gx"] * nz + me["gz"]) * width + o
                    fx, fz = lax.rem(me["gx"] + nx - a, nx), lax.rem(me["gz"] + nz - c, nz)
                    fslot = (fx * nz + fz) * width + o
                    fy = me["gy"] + (o - reach)
                    sidx = (a * nz + c) * width + o

                    def make(tx=tx, tz=tz, ty=ty, slot=slot, sidx=sidx):
                        return pltpu.make_async_remote_copy(
                            src_ref=gsend.at[which], dst_ref=dst_ref.at[slot],
                            send_sem=gss.at[which, sidx], recv_sem=sems.at[slot],
                            device_id={"gx": tx, "gz": tz, "gy": ty}, device_id_type=MESH)

                    def take(tx=tx, tz=tz, ty=ty, fslot=fslot, sidx=sidx):
                        return pltpu.make_async_remote_copy(
                            src_ref=gsend.at[which], dst_ref=dst_ref.at[fslot],
                            send_sem=gss.at[which, sidx], recv_sem=sems.at[fslot],
                            device_id={"gx": tx, "gz": tz, "gy": ty}, device_id_type=MESH)

                    out.append(((ty >= 0) & (ty < ny), make, (fy >= 0) & (fy < ny), take))
        return out

    def gather_start(dst_ref, sems, which):
        for ok, make, _, _ in gather_copies(dst_ref, sems, which):
            @pl.when(ok)
            def _(make=make):
                make().start()
        dst_ref[(me["gx"] * nz + me["gz"]) * width + reach] = gsend[which]

    def gather_finish(dst_ref, sems, which):
        for ok, make, okr, take in gather_copies(dst_ref, sems, which):
            @pl.when(okr)
            def _(take=take):
                take().wait_recv()

            @pl.when(ok)
            def _(make=make):
                make().wait_send()

    def gather_clear(dst_ref):
        for o in range(width):
            fy = me["gy"] + (o - reach)

            @pl.when((fy < 0) | (fy >= ny))
            def _(o=o):
                for s in range(nx * nz):
                    dst_ref[s * width + o] = jnp.zeros((rows2, LANES), F32)

    def unpack(src_ref, out_ref, lead):
        lane = iota((rows2, LANES), 1)
        for sx in range(nx):
            for sz in range(nz):
                tiles = [src_ref[(sx * nz + sz) * width + o] for o in range(width)]
                for p in range(lead):
                    t = jnp.zeros((rows2, LANES), F32)
                    for o in range(width):
                        t = jnp.where(lane // Yc == o, pltpu.roll(tiles[o], ((o - p) * Yc) % LANES, 1), t)
                    for x in range(Xc):
                        out_ref[p, sx * Xc + x, pl.ds(sz * Zc, Zc), :] = t[x * Zc : (x + 1) * Zc]

    def slot_of(x, z, y):
        return (x * nz + z) * ny + y

    def reduce_copies(which, mine_slot):
        out = []
        for a in range(nx):
            for c in range(nz):
                for o in range(ny):
                    if (a, c, o) == (0, 0, 0):
                        continue
                    t = {"gx": lax.rem(me["gx"] + a, nx), "gz": lax.rem(me["gz"] + c, nz),
                         "gy": lax.rem(me["gy"] + o, ny)}
                    f = slot_of(lax.rem(me["gx"] + nx - a, nx), lax.rem(me["gz"] + nz - c, nz),
                                lax.rem(me["gy"] + ny - o, ny))
                    slot = f if not mine_slot else slot_of(me["gx"], me["gz"], me["gy"])
                    out.append(pltpu.make_async_remote_copy(
                        src_ref=asend.at[which], dst_ref=arecv.at[which, slot],
                        send_sem=ass.at[which, slot_of(a, c, o)], recv_sem=ars.at[which, slot],
                        device_id=t, device_id_type=MESH))
        return out

    def reduce_start(which, row):
        asend[which] = row
        for cp in reduce_copies(which, True):
            cp.start()
        arecv[which, slot_of(me["gx"], me["gz"], me["gy"])] = row

    def reduce_finish(which):
        for cp in reduce_copies(which, False):
            cp.wait_recv()
            cp.wait_send()
        return jnp.sum(arecv[which], axis=0)

    lane1 = iota((1, LANES), 1)

    def whole(f):
        s = jnp.sum(f, axis=0)
        return jnp.sum(jnp.sum(s, axis=0, keepdims=True), axis=1, keepdims=True)

    def put(row, q, p, f):
        return jnp.where(lane1 == q * probes + p, whole(f), row)

    def get(row, q, p):
        return jnp.sum(jnp.where(lane1 == q * probes + p, row, 0.0), axis=1, keepdims=True)

    for level in (0, 1):
        for ai, axis in enumerate(AXES):
            for side in (0, 1):
                @pl.when(me[axis] == (0 if side == 0 else counts[axis] - 1))
                def _(level=level, ai=ai, side=side):
                    ref = (xr, zr, yr)[ai][level]
                    for par in (0, 1):
                        ref[par, side] = jnp.zeros(ref.shape[2:], F32)
        zero(ys[level])
    gather_clear(gk)
    for i in (0, 1):
        gather_clear(gr.at[i])

    X0, Z0, Y0 = sizes[0]
    X1, Z1, Y1 = sizes[1]
    k0 = kappa[...]
    d0[...] = k0 + 6.0
    w0[...] = DAMP / d0[...]
    k1 = pool(k0).reshape(X1, Z1, LANES)
    lv1 = iota((X1, Z1, LANES), 2) < Y1
    dd1 = k1 + 6.0 * coup[1]
    d1[...] = dd1
    w1[...] = jnp.where(lv1, DAMP / dd1, 0.0)
    gsend[2] = pool(k1)
    gather_start(gk, gks, 2)

    def first(rhs):
        par = steps[0] % 2

        def fn(p):
            pack(0, par, v0, w0[...] * rhs[p], p)
        return fn

    XG, ZG = nx * Xc, nz * Zc
    WY = width * Yc

    def coefs2():
        gather_finish(gk, gks, 2)
        unpack(gk, k2, 1)
        kk = k2[0]
        lane = iota(kk.shape, 2)
        gy0 = lane + (me["gy"] - reach) * Yc
        ok = (lane < WY) & (gy0 >= 0) & (gy0 < ny * Yc)
        dd = kk + 6.0 * coup[2]
        d2[...] = dd
        w2[...] = jnp.where(ok, DAMP / dd, 0.0)
        kc = pool(kk).reshape(XG // 2, ZG // 2, LANES)
        lane = iota(kc.shape, 2)
        gy0 = lane + (me["gy"] - reach) * (Yc // 2)
        ok = (lane < WY // 2) & (gy0 >= 0) & (gy0 < ny * (Yc // 2))
        k3[...] = jnp.where(ok, DAMP / (kc + 6.0 * coup[3]), 0.0)

    def coarse_part(which):
        src = gr.at[which]
        unpack(src, b2, probes)

        def down2(p):
            b = b2[p]
            w = w2[...]
            v = w * b
            v = (1.0 - DAMP) * v + w * (b + coup[2] * flat_near(v, WY))
            v2[p] = v
            r = b - d2[...] * v + coup[2] * flat_near(v, WY)
            r = jnp.where(w > 0.0, r, 0.0)
            c3[p] = pool(r).reshape(XG // 2, ZG // 2, LANES)
        per_probe(down2)
        w3 = k3[...]
        us = [w3 * c3[p] for p in range(probes)]
        for _ in range(COARSE_SWEEPS - 1):
            us = [(1.0 - DAMP) * u + w3 * (c3[p] + coup[3] * flat_near(u, WY // 2))
                  for p, u in enumerate(us)]
        for p in range(probes):
            c3[p] = us[p]

        def up2(p):
            b = b2[p]
            w = w2[...]
            e = spread(c3[p].reshape(XG // 2 * (ZG // 2), LANES), XG // 2, ZG // 2, spread_m)
            v = v2[p] + jnp.where(w > 0.0, e, 0.0)
            for _ in range(2):
                v = (1.0 - DAMP) * v + w * (b + coup[2] * flat_near(v, WY))
            v2[p] = v
        per_probe(up2)

    def sweep(level, rhs, field, more=True):
        d, w = (d0, d1)[level], (w0, w1)[level]

        def inner(p, v, n):
            return (1.0 - DAMP) * v + w[...] * (rhs[p] + coup[level] * n)
        par = exchange(level, field, inner)
        nxt = steps[level] % 2

        def fn(p):
            v = acc[level][p] + w[...] * (coup[level] * halo(level, par, p))
            if more:
                pack(level, nxt, field, v, p, level == 0)
            else:
                field[p] = v
        per_probe(fn, level == 1)
        if more and level == 1:
            start(level, nxt, field, (0, 1))

    def vcycle(rhs, which):
        per_probe(first(rhs))
        sweep(0, rhs, v0)
        par = exchange(0, v0, lambda p, v, n: rhs[p] - d0[...] * v + n)
        par1 = steps[1] % 2

        def down(p, par=par):
            r = acc[0][p] + halo(0, par, p)
            b = pool(r).reshape(X1, Z1, LANES)
            b1[p] = b
            pack(1, par1, v1, w1[...] * b, p)
        per_probe(down)
        sweep(1, b1, v1)
        par = exchange(1, v1, lambda p, v, n: b1[p] - d1[...] * v + coup[1] * n)
        rows = []

        def down1(p, par=par):
            r = acc[1][p] + coup[1] * halo(1, par, p)
            r = jnp.where(lv1, r, 0.0)
            rows.append(pltpu.roll(pool(r, p), p * Yc, 1))
        per_probe(down1, True)
        gsend[which] = functools.reduce(jnp.add, rows)
        gather_start(gr.at[which], grs.at[which], which)
        if which == 0:
            coefs2()
        gather_finish(gr.at[which], grs.at[which], which)
        coarse_part(which)
        nxt = steps[1] % 2

        def up1(p):
            for x in range(Xc):
                e3[p, pl.ds(x * Zc, Zc), :] = v2[p, me["gx"] * Xc + x, pl.ds(me["gz"] * Zc, Zc), :]
            v = v1[p] + spread(e3[p], Xc, Zc, own_m, p)
            pack(1, nxt, v1, v, p, False)
        per_probe(up1, True)
        start(1, nxt, v1, (0, 1))
        sweep(1, b1, v1)
        sweep(1, b1, v1, more=False)
        nxt0 = steps[0] % 2

        def up0(p):
            v = v0[p] + spread(v1[p].reshape(X1 * Z1, LANES), X1, Z1, spread_m)
            pack(0, nxt0, v0, v, p)
        per_probe(up0)
        sweep(0, rhs, v0)
        sweep(0, rhs, v0, more=which == 0)

    def begin(p):
        r0[p] = 2.0 * bits[p].astype(F32) - 1.0
    per_probe(begin)
    vcycle(r0, 0)
    par = exchange(0, v0, lambda p, v, n: d0[...] * v - n)

    def image(p, row, par=par):
        v = v0[p]
        q = acc[0][p] - halo(0, par, p)
        p0[p] = v
        q0[p] = q
        row = put(row, 0, p, r0[p] * v)
        return put(row, 1, p, v * q)
    row = lax.fori_loop(0, probes, image, jnp.zeros((1, LANES), F32))
    reduce_start(0, row)
    vcycle(q0, 1)
    sums0 = reduce_finish(0)
    nxt = steps[0] % 2

    def direction(p):
        a = get(sums0, 0, p) / get(sums0, 1, p)
        v = p0[p] - a * v0[p]
        r0[p] = r0[p] - a * q0[p]
        pack(0, nxt, v0, v, p)
    per_probe(direction)
    par = exchange(0, v0, lambda p, v, n: d0[...] * v - n)

    def image2(p, row, par=par):
        v = v0[p]
        t = acc[0][p] - halo(0, par, p)
        b0[p] = t
        r, q = r0[p], q0[p]
        a = get(sums0, 0, p) / get(sums0, 1, p)
        g = r - a * t
        for k, f in enumerate((r * v, v * t, v * q, g * g, g * t, g * q, t * t, t * q, q * q)):
            row = put(row, k, p, f)
        return row
    row = lax.fori_loop(0, probes, image2, jnp.zeros((1, LANES), F32))
    reduce_start(1, row)
    sums1 = reduce_finish(1)

    def final(p, row):
        rz0, pq0 = get(sums0, 0, p), get(sums0, 1, p)
        rz1, pt, pq = get(sums1, 0, p), get(sums1, 1, p), get(sums1, 2, p)
        gg, gt, gq, tt, tq, qq = [get(sums1, k, p) for k in range(3, 9)]
        a0 = rz0 / pq0
        beta = rz1 / rz0
        a1 = rz1 / (pt + 2.0 * beta * pq + beta * beta * pq0)
        x_out[p] = a0 * p0[p] + a1 * (v0[p] + beta * p0[p])
        c, h = a1 - a0, a1 * beta
        sq = gg - 2.0 * c * gt - 2.0 * h * gq + c * c * tt + 2.0 * c * h * tq + h * h * qq
        return jnp.where(lane1 == p, sq, row)
    row = lax.fori_loop(0, probes, final, jnp.zeros((1, LANES), F32))
    cells = float(X0 * Z0 * Y0 * total)
    rel_out[...] = jnp.sqrt(jnp.maximum(row, 0.0) / cells)


def per_device(mesh_counts, kappa_sq, probe_bits):
    probes, X, Z, Y = probe_bits.shape
    sizes = [(X >> l, Z >> l, Y >> l) for l in range(LEVELS + 1)]
    need = 2 * (1 + COARSE_SWEEPS - 1) + 2
    reach = min(math.ceil(need / sizes[2][2]), mesh_counts["gy"] - 1)
    width = 2 * reach + 1
    assert Y <= LANES and width * sizes[2][2] <= LANES and probes * X <= LANES
    assert probes * sizes[2][2] <= LANES and 9 * probes <= LANES
    nx, nz, ny = mesh_counts["gx"], mesh_counts["gz"], mesh_counts["gy"]
    total = nx * nz * ny
    slots = nx * nz * width
    Xc, Zc, Yc = sizes[2]
    XG, ZG = nx * Xc, nz * Zc

    def vm(*shape):
        return pltpu.VMEM(shape, F32)

    def full(level):
        return vm(probes, sizes[level][0], sizes[level][1], LANES)

    def coef(level):
        return vm(sizes[level][0], sizes[level][1], LANES)

    def halo(level):
        x, z, _ = sizes[level]
        return [vm(2, 2, probes, z, LANES), vm(2, 2, probes, x, 1, LANES),
                vm(2, 2, probes, x, 1, LANES), vm(2, z, LANES), vm(2, 2, z, LANES), vm(z, LANES)]

    dma = pltpu.SemaphoreType.DMA
    scratch = [full(0), full(0), full(0), full(0), full(0), coef(0), coef(0),
               full(1), full(1), coef(1), coef(1), *halo(0), *halo(1),
               dma((2, 2, 3, 2)), dma((2, 2, 3, 2)),
               vm(probes, max(X * Z, XG * ZG), LANES), vm(3, Xc * Zc, LANES),
               vm(slots, Xc * Zc, LANES), vm(2, slots, Xc * Zc, LANES),
               dma((3, slots)), dma((slots,)), dma((2, slots)),
               vm(probes, XG, ZG, LANES), vm(probes, XG, ZG, LANES), vm(1, XG, ZG, LANES),
               vm(XG, ZG, LANES), vm(probes, XG // 2, ZG // 2, LANES), vm(XG, ZG, LANES),
               vm(XG // 2, ZG // 2, LANES), vm(probes, Xc * Zc, LANES),
               vm(probes, XG // 2, ZG // 2, LANES), full(1),
               vm(2, 1, LANES), vm(2, total, 1, LANES), dma((2, total)), dma((2, total))]
    cfg = (probes, sizes, mesh_counts, reach, width)
    field, rel = pl.pallas_call(
        functools.partial(body, cfg),
        out_shape=(jax.ShapeDtypeStruct(probe_bits.shape, F32),
                   jax.ShapeDtypeStruct((1, LANES), F32)),
        in_specs=[pl.BlockSpec(memory_space=pltpu.VMEM)] * 2,
        out_specs=(pl.BlockSpec(memory_space=pltpu.VMEM),) * 2,
        scratch_shapes=scratch,
        compiler_params=pltpu.CompilerParams(has_side_effects=True, vmem_limit_bytes=48 * 2**20),
    )(kappa_sq, probe_bits)
    return field, rel[0, :probes]


def solution(mesh):
    return jax.shard_map(
        functools.partial(per_device, dict(mesh.shape)),
        mesh=mesh,
        in_specs=(P("gx", "gz", "gy"), P(None, "gx", "gz", "gy")),
        out_specs=(P(None, "gx", "gz", "gy"), P()),
        check_vma=False,
    )
```
